32 devices in a mesh: head: 8 (over y, x, core), level: 4 (over z).
Axes of the slice: x: 2, y: 2, z: 4, core: 2. Of those that a mesh axis runs over, the one named last changes fastest.
Arguments:
- features: float32 [64, 4096], P(None, ('head', 'level')), may hold values from -6 to 6
- in_gain: float32 [4096], replicated, may hold values from 0.25 to 1.75
- in_weight: bfloat16 [4096, 4288], P(None, 'head'), may hold values from -0.09375 to 0.09375
- level_bias: float32 [8, 24], P('head'), may hold values from -4 to 252
- states: bfloat16 [64, 8, 24, 128, 128], P(None, 'head', 'level'), may hold values from -1.25 to 1.25
- positions: int32 [64], replicated, may hold values from 1 to 262143
- out_gain: float32 [1024], P('head'), may hold values from 0.25 to 1.75
- out_weight: bfloat16 [1024, 4096], P('head', 'level'), may hold values from -0.1875 to 0.1875
Outputs:
- output: float32 [64, 4096], P('head', 'level')
The draws below stay inside these ranges and needn't reach their ends.
Inputs may be any that keep to these rules, and one draw needn't show every extreme that they name: `positions`: positions below 2 ** 18, so levels from 19 on are never occupied.
All inputs are finite; a program needn't handle non-finite values.
Results may differ from the reference program's by a relative error of at most 0.0066.
Values sent between devices are 32-bit elements; how exact they have to be, the bound alone decides.
A program may use at most 64 MiB of HBM per device.

```python
import jax
import jax.numpy as jnp
from jax import lax

WIDTH = 4096
HEADS = 8
KEY_DIM = 128
VAL_DIM = 128
LEVELS = 24
PROJ = 536
SEQS = 64


def draw_level_bias(key, part):
    first = jax.random.fold_in(jax.random.fold_in(key, 7), 0)
    return jnp.clip(jax.random.normal(first, (HEADS, LEVELS), jnp.float32), -4.0, 4.0)


def plant(result, stream_key, smallest, top_value):
    place = [jax.random.randint(jax.random.fold_in(stream_key, axis), (), 0, length) for axis, length in enumerate(result.shape)]
    widest = result.shape.index(max(result.shape))
    neighbour = place[:widest] + [(place[widest] + 1) % result.shape[widest]] + place[widest + 1:]
    return result.at[tuple(place)].set(smallest).at[tuple(neighbour)].set(top_value)


def steps_of(rng, shape, cuts, low, high):
    level, own = 1.0, jax.random.fold_in(rng, 6)
    for axis_at, parts in cuts:
        heights = jnp.exp(jax.random.uniform(jax.random.fold_in(own, axis_at), (parts,), jnp.float32, low / len(cuts), high / len(cuts)))
        level = level * jnp.repeat(heights, shape[axis_at] // parts).reshape([-1 if axis == axis_at else 1 for axis in range(len(shape))])
    return level


def noise(stream_key, shape, spread, most, cuts=(), kind=jnp.bfloat16):
    level = steps_of(stream_key, shape, cuts, -0.22, 0.18) if cuts else 1.0
    array = jax.random.normal(stream_key, shape, jnp.float32) * spread * level
    return jnp.minimum(jnp.maximum(array, -most), most).astype(kind)


def setup_inputs(seed: int = 0) -> dict:
    arg_keys = jax.random.split(jax.random.key(seed), 9)
    return {
        "features": noise(arg_keys[0], (SEQS, WIDTH), 1.0, 6.0, ((1, 32),), jnp.float32),
        "in_gain": jnp.clip(1.0 + 0.15 * jax.random.normal(arg_keys[1], (WIDTH,), jnp.float32), 0.25, 1.75),
        "in_weight": noise(arg_keys[2], (WIDTH, HEADS * PROJ), WIDTH ** -0.5, 0.09375, ((1, 8),)),
        "level_bias": draw_level_bias(jax.random.fold_in(arg_keys[8], 71), 0),
        "states": noise(arg_keys[4], (SEQS, HEADS, LEVELS, KEY_DIM, VAL_DIM), (KEY_DIM ** -0.5), 1.25, ((1, 8), (2, 4))),
        "positions": plant(jax.random.randint(arg_keys[5], (SEQS,), 1, 262144), jax.random.fold_in(arg_keys[5], 1), 1, 262143).astype(jnp.int32),
        "out_gain": jnp.clip(1.0 + 0.15 * jax.random.normal(arg_keys[6], (HEADS * VAL_DIM,), jnp.float32), 0.25, 1.75),
        "out_weight": noise(arg_keys[7], (HEADS * VAL_DIM, WIDTH), (HEADS * VAL_DIM) ** -0.5, 0.1875, ((0, 8), (1, 4))),
    }


def occupancy(positions, level_ids):
    shifted = jnp.right_shift(positions[:, None], jnp.maximum(level_ids - 1, 0)[None, :])
    bits = jnp.bitwise_and(shifted, 1).astype(jnp.int32)
    first = (level_ids[None, :] == 0).astype(jnp.int32)
    return jnp.maximum(first, bits)[:, None, :]

def reference(features, in_gain, in_weight, level_bias, states, positions, out_gain, out_weight):
    squares = lax.optimization_barrier(jnp.sum(features * features, axis=1))
    row_scale = lax.rsqrt(squares / WIDTH + 1e-06)
    scaled = (features * in_gain).astype(jnp.bfloat16)
    projected = jnp.dot(scaled, in_weight, preferred_element_type=jnp.float32) * row_scale[:, None]
    projected = projected.reshape(SEQS, HEADS, PROJ)
    query_vec = projected[:, :, :KEY_DIM]
    key_vec = projected[:, :, KEY_DIM:2 * KEY_DIM]
    value_vec = projected[:, :, 2 * KEY_DIM:2 * KEY_DIM + VAL_DIM]
    gate_vec = projected[:, :, 2 * KEY_DIM + VAL_DIM:2 * KEY_DIM + 2 * VAL_DIM]
    logits = projected[:, :, 2 * KEY_DIM + 2 * VAL_DIM:] + level_bias[None]
    level_ids = jnp.arange(LEVELS, dtype=jnp.int32)
    occupied = occupancy(positions, level_ids) == 1
    peak_logit = lax.optimization_barrier(jnp.max(jnp.where(occupied, logits, -1e+30), axis=2, keepdims=True))
    weights = jnp.where(occupied, jnp.exp(logits - peak_logit), 0.0)
    total_weight = lax.optimization_barrier(jnp.sum(weights, axis=2))
    query_low = query_vec.astype(jnp.bfloat16)

    def read_head(head_id):
        query_head = lax.dynamic_index_in_dim(query_low, head_id, 1, keepdims=False).astype(jnp.float32)
        state_head = lax.dynamic_index_in_dim(states, head_id, 1, keepdims=False).astype(jnp.float32)
        return jnp.einsum('bk,blkv->blv', query_head, state_head)
    reads = lax.map(read_head, jnp.arange(HEADS, dtype=jnp.int32))
    reads = jnp.transpose(reads, (1, 0, 2, 3))
    own_term = lax.optimization_barrier(jnp.sum(query_vec * key_vec, axis=2, keepdims=True)) * KEY_DIM ** (-0.5) * value_vec
    mixed = lax.optimization_barrier(jnp.sum(weights[..., None] * reads, axis=2)) + weights[:, :, :1] * own_term
    level_out = mixed / total_weight[..., None]
    gated = (level_out * jax.nn.silu(gate_vec)).reshape(SEQS, HEADS * VAL_DIM)
    mean_square = lax.optimization_barrier(jnp.mean(gated * gated, axis=1, keepdims=True))
    normed = (gated * lax.rsqrt(mean_square + 1e-05) * out_gain).astype(jnp.bfloat16)
    return jnp.dot(normed, out_weight, preferred_element_type=jnp.float32)
```

```python
import functools

import jax
import jax.numpy as jnp
from jax import lax
from jax.experimental import pallas as pl
from jax.experimental.pallas import tpu as pltpu
from jax.sharding import PartitionSpec as P

LANES = 128
GROUP = 16


def send(src, dst, send_sem, recv_sem, target):
    return pltpu.make_async_remote_copy(
        src_ref=src,
        dst_ref=dst,
        send_sem=send_sem,
        recv_sem=recv_sem,
        device_id=target,
        device_id_type=pl.DeviceIdType.MESH,
    )


def kernel(
    heads, levels, width, dims,
    feat, gain, inw, bias, states, pos, ogain, outw, out,
    xbuf, wbuf, sbuf, owbuf, proj, abuf, bbuf, mbuf, osend, orecv, qfull, wnorm, qw, biasbuf,
    x_sem, w_sem, s_sem, ow_sem, p1_send, p1_recv, a_send, a_recv, b_send, b_recv,
    m_send, m_recv, o_send, o_recv,
):
    key_dim, val_dim, level_total, level_here = dims
    seqs, fw = feat.shape
    flipped = fw % LANES == 0
    cols = inw.shape[0] if flipped else inw.shape[1]
    owned = seqs // levels
    out_rows = seqs // heads
    out_cols = outw.shape[1]
    me_h, me_l = lax.axis_index("head"), lax.axis_index("level")
    slot = 1 << level_total.bit_length()
    slots = LANES // slot
    packed = seqs // slots
    groups = seqs // GROUP

    x_copy = pltpu.make_async_copy(feat, xbuf.at[me_h], x_sem)
    x_copy.start()
    w_copies = []
    for h in range(heads):
        start = pl.multiple_of((h * levels + me_l) * fw, fw)
        part = inw.at[:, pl.ds(start, fw)] if flipped else inw.at[pl.ds(start, fw), :]
        w_copies.append(pltpu.make_async_copy(part, wbuf.at[h], w_sem.at[h]))
        w_copies[-1].start()
    s_copies = []
    for g in range(groups):
        rows = pl.ds(g * GROUP, GROUP)
        s_copies.append(pltpu.make_async_copy(states.at[rows], sbuf.at[rows], s_sem.at[g]))
        s_copies[-1].start()
    ow_copy = pltpu.make_async_copy(outw, owbuf, ow_sem)
    ow_copy.start()

    barrier = pltpu.get_barrier_semaphore()
    for o in range(1, heads):
        pl.semaphore_signal(
            barrier, inc=1, device_id=(lax.rem(me_h + o, heads), me_l),
            device_id_type=pl.DeviceIdType.MESH)
    for o in range(1, levels):
        pl.semaphore_signal(
            barrier, inc=1, device_id=(me_h, lax.rem(me_l + o, levels)),
            device_id_type=pl.DeviceIdType.MESH)
    pl.semaphore_wait(barrier, heads + levels - 2)

    x_copy.wait()
    pending = []
    for o in range(1, heads):
        peer = lax.rem(me_h + o, heads)
        c = send(xbuf.at[me_h], xbuf.at[me_h], p1_send.at[o], p1_recv.at[me_h], (peer, me_l))
        c.start()
        pending.append(c)

    for c in w_copies:
        c.wait()
    acc = jnp.zeros((seqs, cols), jnp.float32)
    squares = jnp.zeros((seqs, 1), jnp.float32)
    for o in range(heads):
        src = lax.rem(me_h + heads - o, heads)
        if o:
            send(xbuf.at[src], xbuf.at[src], p1_send.at[o], p1_recv.at[src], (src, me_l)).wait_recv()
        x = xbuf[src]
        g = gain[pl.ds(src * levels + me_l, 1), :]
        acc += lax.dot_general(
            (x * g).astype(jnp.bfloat16), wbuf[src], (((1,), (1 if flipped else 0,)), ((), ())),
            preferred_element_type=jnp.float32)
        squares += jnp.sum(x * x, axis=1, keepdims=True)

    proj[:, :cols] = acc
    lane = lax.broadcasted_iota(jnp.int32, (seqs, LANES), 1)
    tail0 = 2 * key_dim + 2 * val_dim
    tail = jnp.where(lane < level_total, proj[:, tail0 : tail0 + LANES], 0.0)
    tail = jnp.where(lane == level_total, squares, tail)
    pack = tail[:packed]
    for c in range(1, slots):
        pack += pltpu.roll(tail[c * packed : (c + 1) * packed], slot * c, 1)
    abuf[me_l, :seqs, :] = acc[:, :key_dim]
    abuf[me_l, seqs:, :] = pack
    for o in range(1, levels):
        peer = lax.rem(me_l + o, levels)
        c = send(abuf.at[me_l], abuf.at[me_l], a_send.at[o], a_recv.at[me_l], (me_h, peer))
        c.start()
        pending.append(c)
    for o in range(1, levels):
        peer = lax.rem(me_l + o, levels)
        rows = pl.ds(pl.multiple_of(peer * owned, owned), owned)
        c = send(proj.at[rows, pl.ds(key_dim, tail0 - key_dim)], bbuf.at[me_l],
                 b_send.at[o], b_recv.at[me_l], (me_h, peer))
        c.start()
        pending.append(c)
    mine = pl.ds(pl.multiple_of(me_l * owned, owned), owned)
    bbuf[me_l] = proj[mine, key_dim:tail0]

    biasbuf[:, :level_total] = bias[...]
    row = lax.broadcasted_iota(jnp.int32, (seqs, seqs), 0)
    col = lax.broadcasted_iota(jnp.int32, (seqs, seqs), 1)
    pos_f = jnp.broadcast_to(pos[...], (seqs, seqs)).astype(jnp.float32)
    pos_col = jnp.sum(jnp.where(row == col, pos_f, 0.0), axis=1, keepdims=True).astype(jnp.int32)
    shift = jnp.clip(lane - 1, 0, 31)
    bits = jnp.bitwise_and(jnp.right_shift(jnp.broadcast_to(pos_col, lane.shape), shift), 1)
    occupied = jnp.logical_and(lane < level_total, jnp.logical_or(lane == 0, bits == 1))

    for o in range(1, levels):
        src = lax.rem(me_l + levels - o, levels)
        send(abuf.at[src], abuf.at[src], a_send.at[o], a_recv.at[src], (me_h, src)).wait_recv()
    query = abuf[0, :seqs, :]
    pack = abuf[0, seqs:, :]
    for l in range(1, levels):
        query += abuf[l, :seqs, :]
        pack += abuf[l, seqs:, :]
    parts = [pack] + [pltpu.roll(pack, LANES - slot * c, 1) for c in range(1, slots)]
    tail = jnp.concatenate(parts, axis=0)
    row_scale = lax.rsqrt(tail[:, level_total : level_total + 1] / width + 1e-06)
    query = query * row_scale
    logits = tail * row_scale + biasbuf[...]
    peak = jnp.max(jnp.where(occupied, logits, -1e30), axis=1, keepdims=True)
    weights = jnp.where(occupied, jnp.exp(logits - peak), 0.0)
    weights = weights / jnp.sum(weights, axis=1, keepdims=True)
    qfull[...] = query
    wnorm[:, :LANES] = weights
    wnorm[:, LANES:] = jnp.broadcast_to(row_scale, weights.shape)
    local = pltpu.roll(weights, lax.rem(LANES - me_l * level_here, LANES), 1)
    query_low = query.astype(jnp.bfloat16).astype(jnp.float32)
    for j in range(level_here):
        qw[:, j * key_dim : (j + 1) * key_dim] = (query_low * local[:, j : j + 1]).astype(jnp.bfloat16)

    seq_in = lax.broadcasted_iota(jnp.int32, (GROUP, val_dim), 0)
    for g in range(groups):
        s_copies[g].wait()
    def read_group(g, carry):
        base = pl.multiple_of(g * GROUP, GROUP)
        left = qw[pl.ds(base, GROUP), :]
        mixed = jnp.zeros((GROUP, val_dim), jnp.float32)
        for i in range(GROUP):
            got = jnp.dot(left, sbuf[base + i], preferred_element_type=jnp.float32)
            mixed = jnp.where(seq_in == i, got, mixed)
        mbuf[me_l, pl.ds(base, GROUP), :] = mixed
        return carry
    lax.fori_loop(0, groups, read_group, 0)

    for o in range(1, levels):
        src = lax.rem(me_l + levels - o, levels)
        send(bbuf.at[src], bbuf.at[src], b_send.at[o], b_recv.at[src], (me_h, src)).wait_recv()
    rest = bbuf[0]
    for l in range(1, levels):
        rest += bbuf[l]
    rest = rest * wnorm[mine, LANES : LANES + 1]
    key, value = rest[:, :key_dim], rest[:, key_dim : key_dim + val_dim]
    gate = rest[:, key_dim + val_dim :]
    own = jnp.sum(qfull[mine, :] * key, axis=1, keepdims=True) * key_dim ** (-0.5) * value
    mbuf[me_l, mine, :] = mbuf[me_l, mine, :] + wnorm[mine, 0:1] * own
    mbuf[me_l, seqs:, :] = gate * jax.nn.sigmoid(gate)
    for o in range(1, levels):
        peer = lax.rem(me_l + o, levels)
        c = send(mbuf.at[me_l], mbuf.at[me_l], m_send.at[o], m_recv.at[me_l], (me_h, peer))
        c.start()
        pending.append(c)
    ow_copy.wait()
    for o in range(1, levels):
        src = lax.rem(me_l + levels - o, levels)
        send(mbuf.at[src], mbuf.at[src], m_send.at[o], m_recv.at[src], (me_h, src)).wait_recv()
    gated = mbuf[0, :seqs, :]
    for l in range(1, levels):
        gated += mbuf[l, :seqs, :]
    gated = gated * jnp.concatenate([mbuf[l, seqs:, :] for l in range(levels)], axis=0)
    total_sq = jnp.sum(gated * gated, axis=1, keepdims=True)
    product = jnp.dot((gated * ogain[...]).astype(jnp.bfloat16), owbuf[...], preferred_element_type=jnp.float32)
    wide_sq = jnp.broadcast_to(total_sq, (seqs, LANES))
    for h in range(heads):
        osend[h, :, :out_cols] = product[h * out_rows : (h + 1) * out_rows]
        osend[h, :, out_cols:] = wide_sq[h * out_rows : (h + 1) * out_rows]
    for o in range(1, heads):
        peer = lax.rem(me_h + o, heads)
        c = send(osend.at[peer], orecv.at[me_h], o_send.at[o], o_recv.at[me_h], (peer, me_l))
        c.start()
        pending.append(c)
    total = osend[me_h]
    for o in range(1, heads):
        src = lax.rem(me_h + heads - o, heads)
        send(osend.at[src], orecv.at[src], o_send.at[o], o_recv.at[src], (src, me_l)).wait_recv()
        total += orecv[src]
    mean = total[:, out_cols : out_cols + 1] / (heads * val_dim)
    out[...] = total[:, :out_cols] * lax.rsqrt(mean + 1e-05)
    for c in pending:
        c.wait_send()


def body(features, in_gain, in_weight, level_bias, states, positions, out_gain, out_weight):
    heads, levels = lax.axis_size("head"), lax.axis_size("level")
    seqs, fw = features.shape
    cols = in_weight.shape[1]
    _, head_here, level_here, key_dim, val_dim = states.shape
    level_total = level_bias.shape[1]
    assert head_here == 1 and key_dim == LANES and val_dim == LANES
    out_cols = out_weight.shape[1]
    flipped = fw % LANES == 0
    slots = LANES // (1 << level_total.bit_length())
    owned, out_rows = seqs // levels, seqs // heads
    f32, bf16 = jnp.float32, jnp.bfloat16
    vmem, anyspace = pl.BlockSpec(memory_space=pltpu.VMEM), pl.BlockSpec(memory_space=pl.ANY)
    dma = pltpu.SemaphoreType.DMA
    tail0 = 2 * key_dim + 2 * val_dim
    return pl.pallas_call(
        functools.partial(kernel, heads, levels, in_gain.shape[0], (key_dim, val_dim, level_total, level_here)),
        out_shape=jax.ShapeDtypeStruct((out_rows, out_cols), f32),
        in_specs=[anyspace, vmem, anyspace, vmem, anyspace, vmem, vmem, anyspace],
        out_specs=vmem,
        scratch_shapes=[
            pltpu.VMEM((heads, seqs, fw), f32),
            pltpu.VMEM((heads, cols, fw) if flipped else (heads, fw, cols), bf16),
            pltpu.VMEM((seqs, level_here * key_dim, val_dim), bf16),
            pltpu.VMEM(out_weight.shape, bf16),
            pltpu.VMEM((seqs, tail0 + LANES), f32),
            pltpu.VMEM((levels, seqs + seqs // slots, key_dim), f32),
            pltpu.VMEM((levels, owned, tail0 - key_dim), f32),
            pltpu.VMEM((levels, seqs + owned, val_dim), f32),
            pltpu.VMEM((heads, out_rows, out_cols + LANES), f32),
            pltpu.VMEM((heads, out_rows, out_cols + LANES), f32),
            pltpu.VMEM((seqs, key_dim), f32),
            pltpu.VMEM((seqs, 2 * LANES), f32),
            pltpu.VMEM((seqs, level_here * key_dim), bf16),
            pltpu.VMEM((1, LANES), f32),
            dma(()), dma((heads,)), dma((seqs // GROUP,)), dma(()),
            dma((heads,)), dma((heads,)),
            dma((levels,)), dma((levels,)), dma((levels,)), dma((levels,)),
            dma((levels,)), dma((levels,)),
            dma((heads,)), dma((heads,)),
        ],
        compiler_params=pltpu.CompilerParams(collective_id=0, has_side_effects=True),
    )(
        features,
        in_gain.reshape(heads * levels, fw),
        in_weight.T if flipped else in_weight,
        level_bias,
        states.reshape(seqs, level_here * key_dim, val_dim),
        positions.reshape(1, seqs),
        out_gain.reshape(1, val_dim),
        out_weight,
    )


def solution(mesh):
    in_specs = (
        P(None, ("head", "level")),
        P(),
        P(None, "head"),
        P("head", None),
        P(None, "head", "level", None, None),
        P(),
        P("head"),
        P("head", "level"),
    )
    out_specs = P("head", "level")
    return jax.shard_map(body, mesh=mesh, in_specs=in_specs, out_specs=out_specs, check_vma=False)
```

```python
import functools

import jax
import jax.numpy as jnp
from jax import lax
from jax.experimental import pallas as pl
from jax.experimental.pallas import tpu as pltpu
from jax.sharding import PartitionSpec as P

LANES = 128
GROUP = 16


def send(src, dst, send_sem, recv_sem, target):
    return pltpu.make_async_remote_copy(
        src_ref=src,
        dst_ref=dst,
        send_sem=send_sem,
        recv_sem=recv_sem,
        device_id=target,
        device_id_type=pl.DeviceIdType.MESH,
    )


def kernel(
    heads, levels, width, dims,
    feat, gain, inw, bias, states, pos, ogain, outw, out,
    xbuf, wbuf, sbuf, owbuf, proj, abuf, bbuf, mbuf, osend, orecv, qfull, wnorm, qw, biasbuf,
    x_sem, w_sem, s_sem, ow_sem, p1_send, p1_recv, a_send, a_recv, b_send, b_recv,
    m_send, m_recv, o_send, o_recv,
):
    key_dim, val_dim, level_total, level_here = dims
    seqs, fw = feat.shape
    flipped = fw % LANES == 0
    cols = inw.shape[0] if flipped else inw.shape[1]
    owned = seqs // levels
    out_rows = seqs // heads
    out_cols = outw.shape[1]
    me_h, me_l = lax.axis_index("head"), lax.axis_index("level")
    slot = 1 << level_total.bit_length()
    slots = LANES // slot
    packed = seqs // slots
    groups = seqs // GROUP

    x_copy = pltpu.make_async_copy(feat, xbuf.at[me_h], x_sem)
    x_copy.start()
    w_copies = []
    for h in range(heads):
        start = pl.multiple_of((h * levels + me_l) * fw, fw)
        part = inw.at[:, pl.ds(start, fw)] if flipped else inw.at[pl.ds(start, fw), :]
        w_copies.append(pltpu.make_async_copy(part, wbuf.at[h], w_sem.at[h]))
        w_copies[-1].start()
    last_group = (me_l * owned) // GROUP
    order = [lax.rem(last_group + 1 + t, groups) for t in range(groups)]

    def state_copy(g):
        rows = pl.ds(pl.multiple_of(g * GROUP, GROUP), GROUP)
        return pltpu.make_async_copy(states.at[rows], sbuf.at[rows], s_sem.at[g])

    ow_copy = pltpu.make_async_copy(outw, owbuf, ow_sem)

    barrier = pltpu.get_barrier_semaphore()
    for o in range(1, heads):
        pl.semaphore_signal(
            barrier, inc=1, device_id=(lax.rem(me_h + o, heads), me_l),
            device_id_type=pl.DeviceIdType.MESH)
    for o in range(1, levels):
        pl.semaphore_signal(
            barrier, inc=1, device_id=(me_h, lax.rem(me_l + o, levels)),
            device_id_type=pl.DeviceIdType.MESH)
    pl.semaphore_wait(barrier, heads + levels - 2)

    x_copy.wait()
    pending = []
    buddy = me_h + 1 - 2 * lax.rem(me_h, 2)
    def feature_send(block, target, index):
        c = send(xbuf.at[block], xbuf.at[block], p1_send.at[index], p1_recv.at[block], (target, me_l))
        c.start()
        pending.append(c)

    def feature_wait(block):
        send(xbuf.at[block], xbuf.at[block], p1_send.at[0], p1_recv.at[block], (buddy, me_l)).wait_recv()

    same = [lax.rem(me_h + o, heads) for o in range(2, heads, 2)]
    for i, peer in enumerate(same):
        feature_send(me_h, peer, i)
    feature_send(me_h, buddy, heads - 1)
    for c in w_copies:
        c.wait()
    acc = jnp.zeros((seqs, cols), jnp.float32)
    squares = jnp.zeros((seqs, 1), jnp.float32)
    other = [lax.rem(buddy + o, heads) for o in range(2, heads, 2)]
    for i, src in enumerate([me_h, buddy] + same + other):
        if i:
            feature_wait(src)
        if 2 <= i < 2 + len(same):
            feature_send(src, buddy, len(same) + i - 2)
        x = xbuf[src]
        g = gain[pl.ds(src * levels + me_l, 1), :]
        acc += lax.dot_general(
            (x * g).astype(jnp.bfloat16), wbuf[src], (((1,), (1 if flipped else 0,)), ((), ())),
            preferred_element_type=jnp.float32)
        squares += jnp.sum(x * x, axis=1, keepdims=True)

    for g in order:
        state_copy(g).start()
    ow_copy.start()

    proj[:, :cols] = acc
    lane = lax.broadcasted_iota(jnp.int32, (seqs, LANES), 1)
    tail0 = 2 * key_dim + 2 * val_dim
    tail = jnp.where(lane < level_total, proj[:, tail0 : tail0 + LANES], 0.0)
    tail = jnp.where(lane == level_total, squares, tail)
    pack = tail[:packed]
    for c in range(1, slots):
        pack += pltpu.roll(tail[c * packed : (c + 1) * packed], slot * c, 1)
    abuf[me_l, :seqs, :] = acc[:, :key_dim]
    abuf[me_l, seqs:, :] = pack
    for o in range(1, levels):
        peer = lax.rem(me_l + o, levels)
        c = send(abuf.at[me_l], abuf.at[me_l], a_send.at[o], a_recv.at[me_l], (me_h, peer))
        c.start()
        pending.append(c)
    for o in range(1, levels):
        peer = lax.rem(me_l + o, levels)
        rows = pl.ds(pl.multiple_of(peer * owned, owned), owned)
        c = send(proj.at[rows, pl.ds(key_dim, tail0 - key_dim)], bbuf.at[me_l],
                 b_send.at[o], b_recv.at[me_l], (me_h, peer))
        c.start()
        pending.append(c)
    mine = pl.ds(pl.multiple_of(me_l * owned, owned), owned)
    bbuf[me_l] = proj[mine, key_dim:tail0]

    biasbuf[:, :level_total] = bias[...]
    row = lax.broadcasted_iota(jnp.int32, (seqs, seqs), 0)
    col = lax.broadcasted_iota(jnp.int32, (seqs, seqs), 1)
    pos_f = jnp.broadcast_to(pos[...], (seqs, seqs)).astype(jnp.float32)
    pos_col = jnp.sum(jnp.where(row == col, pos_f, 0.0), axis=1, keepdims=True).astype(jnp.int32)
    shift = jnp.clip(lane - 1, 0, 31)
    bits = jnp.bitwise_and(jnp.right_shift(jnp.broadcast_to(pos_col, lane.shape), shift), 1)
    occupied = jnp.logical_and(lane < level_total, jnp.logical_or(lane == 0, bits == 1))

    for o in range(1, levels):
        src = lax.rem(me_l + levels - o, levels)
        send(abuf.at[src], abuf.at[src], a_send.at[o], a_recv.at[src], (me_h, src)).wait_recv()
    query = abuf[0, :seqs, :]
    pack = abuf[0, seqs:, :]
    for l in range(1, levels):
        query += abuf[l, :seqs, :]
        pack += abuf[l, seqs:, :]
    parts = [pack] + [pltpu.roll(pack, LANES - slot * c, 1) for c in range(1, slots)]
    tail = jnp.concatenate(parts, axis=0)
    row_scale = lax.rsqrt(tail[:, level_total : level_total + 1] / width + 1e-06)
    query = query * row_scale
    logits = tail * row_scale + biasbuf[...]
    peak = jnp.max(jnp.where(occupied, logits, -1e30), axis=1, keepdims=True)
    weights = jnp.where(occupied, jnp.exp(logits - peak), 0.0)
    weights = weights / jnp.sum(weights, axis=1, keepdims=True)
    qfull[...] = query
    wnorm[:, :LANES] = weights
    wnorm[:, LANES:] = jnp.broadcast_to(row_scale, weights.shape)
    local = pltpu.roll(weights, lax.rem(LANES - me_l * level_here, LANES), 1)
    query_low = query.astype(jnp.bfloat16).astype(jnp.float32)
    for j in range(level_here):
        qw[:, j * key_dim : (j + 1) * key_dim] = (query_low * local[:, j : j + 1]).astype(jnp.bfloat16)

    seq_in = lax.broadcasted_iota(jnp.int32, (GROUP, val_dim), 0)
    def to_levels(rows, index):
        for o in range(1, levels):
            part = mbuf.at[me_l, rows, :]
            c = send(part, part, m_send.at[o, index], m_recv.at[me_l, index],
                     (me_h, lax.rem(me_l + o, levels)))
            c.start()
            pending.append(c)

    for t, g in enumerate(order):
        if t == groups - 1:
            for o in range(1, levels):
                src = lax.rem(me_l + levels - o, levels)
                send(bbuf.at[src], bbuf.at[src], b_send.at[o], b_recv.at[src], (me_h, src)).wait_recv()
            rest = bbuf[0]
            for l in range(1, levels):
                rest += bbuf[l]
            rest = rest * wnorm[mine, LANES : LANES + 1]
            key, value = rest[:, :key_dim], rest[:, key_dim : key_dim + val_dim]
            gate = rest[:, key_dim + val_dim :]
            own = jnp.sum(qfull[mine, :] * key, axis=1, keepdims=True) * key_dim ** (-0.5) * value
            mbuf[me_l, seqs:, :] = gate * jax.nn.sigmoid(gate)
            to_levels(pl.ds(seqs, owned), groups)
            qfull[...] = jnp.zeros(qfull.shape, jnp.float32)
            qfull[mine, :] = wnorm[mine, 0:1] * own
        state_copy(g).wait()
        base = pl.multiple_of(g * GROUP, GROUP)
        rows = pl.ds(base, GROUP)
        left = qw[rows, :]
        mixed = jnp.zeros((GROUP, val_dim), jnp.float32)
        for i in range(GROUP):
            got = jnp.dot(left, sbuf[base + i], preferred_element_type=jnp.float32)
            mixed = jnp.where(seq_in == i, got, mixed)
        if t == groups - 1:
            mixed += qfull[rows, :]
        mbuf[me_l, rows, :] = mixed
        to_levels(rows, g)
    ow_copy.wait()
    for o in range(1, levels):
        src = lax.rem(me_l + levels - o, levels)
        for index in range(groups + 1):
            rows = pl.ds(index * GROUP, GROUP if index < groups else owned)
            part = mbuf.at[src, rows, :]
            send(part, part, m_send.at[o, index], m_recv.at[src, index], (me_h, src)).wait_recv()
    gated = mbuf[0, :seqs, :]
    for l in range(1, levels):
        gated += mbuf[l, :seqs, :]
    gated = gated * jnp.concatenate([mbuf[l, seqs:, :] for l in range(levels)], axis=0)
    total_sq = jnp.sum(gated * gated, axis=1, keepdims=True)
    product = jnp.dot((gated * ogain[...]).astype(jnp.bfloat16), owbuf[...], preferred_element_type=jnp.float32)
    wide_sq = jnp.broadcast_to(total_sq, (seqs, LANES))
    for h in range(heads):
        osend[h, :, :out_cols] = product[h * out_rows : (h + 1) * out_rows]
        osend[h, :, out_cols:] = wide_sq[h * out_rows : (h + 1) * out_rows]
    for o in range(1, heads):
        peer = lax.rem(me_h + o, heads)
        c = send(osend.at[peer], orecv.at[me_h], o_send.at[o], o_recv.at[me_h], (peer, me_l))
        c.start()
        pending.append(c)
    total = osend[me_h]
    for o in range(1, heads):
        src = lax.rem(me_h + heads - o, heads)
        send(osend.at[src], orecv.at[src], o_send.at[o], o_recv.at[src], (src, me_l)).wait_recv()
        total += orecv[src]
    mean = total[:, out_cols : out_cols + 1] / (heads * val_dim)
    out[...] = total[:, :out_cols] * lax.rsqrt(mean + 1e-05)
    for c in pending:
        c.wait_send()


def body(features, in_gain, in_weight, level_bias, states, positions, out_gain, out_weight):
    heads, levels = lax.axis_size("head"), lax.axis_size("level")
    seqs, fw = features.shape
    cols = in_weight.shape[1]
    _, head_here, level_here, key_dim, val_dim = states.shape
    level_total = level_bias.shape[1]
    assert head_here == 1 and key_dim == LANES and val_dim == LANES
    out_cols = out_weight.shape[1]
    flipped = fw % LANES == 0
    slots = LANES // (1 << level_total.bit_length())
    owned, out_rows = seqs // levels, seqs // heads
    f32, bf16 = jnp.float32, jnp.bfloat16
    vmem, anyspace = pl.BlockSpec(memory_space=pltpu.VMEM), pl.BlockSpec(memory_space=pl.ANY)
    dma = pltpu.SemaphoreType.DMA
    tail0 = 2 * key_dim + 2 * val_dim
    return pl.pallas_call(
        functools.partial(kernel, heads, levels, in_gain.shape[0], (key_dim, val_dim, level_total, level_here)),
        out_shape=pltpu.VMEM((out_rows, out_cols), f32),
        in_specs=[anyspace, vmem, anyspace, vmem, anyspace, vmem, vmem, anyspace],
        out_specs=vmem,
        scratch_shapes=[
            pltpu.VMEM((heads, seqs, fw), f32),
            pltpu.VMEM((heads, cols, fw) if flipped else (heads, fw, cols), bf16),
            pltpu.VMEM((seqs, level_here * key_dim, val_dim), bf16),
            pltpu.VMEM(out_weight.shape, bf16),
            pltpu.VMEM((seqs, tail0 + LANES), f32),
            pltpu.VMEM((levels, seqs + seqs // slots, key_dim), f32),
            pltpu.VMEM((levels, owned, tail0 - key_dim), f32),
            pltpu.VMEM((levels, seqs + owned, val_dim), f32),
            pltpu.VMEM((heads, out_rows, out_cols + LANES), f32),
            pltpu.VMEM((heads, out_rows, out_cols + LANES), f32),
            pltpu.VMEM((seqs, key_dim), f32),
            pltpu.VMEM((seqs, 2 * LANES), f32),
            pltpu.VMEM((seqs, level_here * key_dim), bf16),
            pltpu.VMEM((1, LANES), f32),
            dma(()), dma((heads,)), dma((seqs // GROUP,)), dma(()),
            dma((heads,)), dma((heads,)),
            dma((levels,)), dma((levels,)), dma((levels,)), dma((levels,)),
            dma((levels, seqs // GROUP + 1)), dma((levels, seqs // GROUP + 1)),
            dma((heads,)), dma((heads,)),
        ],
        compiler_params=pltpu.CompilerParams(collective_id=0, has_side_effects=True),
    )(
        features,
        in_gain.reshape(heads * levels, fw),
        in_weight.T if flipped else in_weight,
        level_bias,
        states.reshape(seqs, level_here * key_dim, val_dim),
        positions.reshape(1, seqs),
        out_gain.reshape(1, val_dim),
        out_weight,
    )


def solution(mesh):
    in_specs = (
        P(None, ("head", "level")),
        P(),
        P(None, "head"),
        P("head", None),
        P(None, "head", "level", None, None),
        P(),
        P("head"),
        P("head", "level"),
    )
    out_specs = P("head", "level")
    return jax.shard_map(body, mesh=mesh, in_specs=in_specs, out_specs=out_specs, check_vma=False)
```

```python
import functools

import jax
import jax.numpy as jnp
from jax import lax
from jax.experimental import pallas as pl
from jax.experimental.pallas import tpu as pltpu
from jax.sharding import PartitionSpec as P

LANES = 128
GROUP = 16


def send(src, dst, send_sem, recv_sem, target):
    return pltpu.make_async_remote_copy(
        src_ref=src,
        dst_ref=dst,
        send_sem=send_sem,
        recv_sem=recv_sem,
        device_id=target,
        device_id_type=pl.DeviceIdType.MESH,
    )


def kernel(
    heads, levels, width, dims,
    feat, gain, inw, bias, states, pos, ogain, outw, out,
    xbuf, wbuf, sbuf, owbuf, proj, abuf, bbuf, mbuf, osend, orecv, qfull, wnorm, qw, biasbuf, qsum,
    x_sem, w_sem, s_sem, ow_sem, p1_send, p1_recv, a_send, a_recv, b_send, b_recv,
    m_send, m_recv, o_send, o_recv, q_send, q_recv,
):
    key_dim, val_dim, level_total, level_here = dims
    seqs, fw = feat.shape
    flipped = fw % LANES == 0
    cols = inw.shape[0] if flipped else inw.shape[1]
    owned = seqs // levels
    out_rows = seqs // heads
    out_cols = outw.shape[1]
    me_h, me_l = lax.axis_index("head"), lax.axis_index("level")
    slot = 1 << level_total.bit_length()
    slots = LANES // slot
    packed = seqs // slots
    groups = seqs // GROUP

    x_copy = pltpu.make_async_copy(feat, xbuf.at[me_h], x_sem)
    x_copy.start()
    w_copies = []
    for h in range(heads):
        start = pl.multiple_of((h * levels + me_l) * fw, fw)
        part = inw.at[:, pl.ds(start, fw)] if flipped else inw.at[pl.ds(start, fw), :]
        w_copies.append(pltpu.make_async_copy(part, wbuf.at[h], w_sem.at[h]))
        w_copies[-1].start()
    last_group = (me_l * owned) // GROUP
    order = [lax.rem(last_group + 1 + t, groups) for t in range(groups)]

    def state_copy(g):
        rows = pl.ds(pl.multiple_of(g * GROUP, GROUP), GROUP)
        return pltpu.make_async_copy(states.at[rows], sbuf.at[rows], s_sem.at[g])

    ow_copy = pltpu.make_async_copy(outw, owbuf, ow_sem)

    barrier = pltpu.get_barrier_semaphore()
    for o in range(1, heads):
        pl.semaphore_signal(
            barrier, inc=1, device_id=(lax.rem(me_h + o, heads), me_l),
            device_id_type=pl.DeviceIdType.MESH)
    for o in range(1, levels):
        pl.semaphore_signal(
            barrier, inc=1, device_id=(me_h, lax.rem(me_l + o, levels)),
            device_id_type=pl.DeviceIdType.MESH)
    pl.semaphore_wait(barrier, heads + levels - 2)

    x_copy.wait()
    pending = []
    buddy = me_h + 1 - 2 * lax.rem(me_h, 2)
    def feature_send(block, target, index):
        c = send(xbuf.at[block], xbuf.at[block], p1_send.at[index], p1_recv.at[block], (target, me_l))
        c.start()
        pending.append(c)

    def feature_wait(block):
        send(xbuf.at[block], xbuf.at[block], p1_send.at[0], p1_recv.at[block], (buddy, me_l)).wait_recv()

    chips, core = heads // 2, lax.rem(me_h, 2)
    mirror_chip = chips - 1 - me_h // 2
    skip = lax.rem(me_h // 2 - mirror_chip + chips, chips)
    mirror = 2 * mirror_chip + core
    direct = []
    for j in range(1, chips - 1):
        near = 2 * lax.rem(mirror_chip + j + (j + chips - skip) // chips, chips)
        direct += [near + core, near + 1 - core]
    feature_send(me_h, mirror, heads - 1)
    for i, peer in enumerate(direct):
        feature_send(me_h, peer, i)
    feature_send(me_h, buddy, heads - 2)
    for c in w_copies:
        c.wait()
    acc = jnp.zeros((seqs, cols), jnp.float32)
    squares = jnp.zeros((seqs, 1), jnp.float32)
    arrivals = [me_h, buddy, mirror] + direct + [2 * mirror_chip + 1 - core]
    for i, src in enumerate(arrivals):
        if i:
            feature_wait(src)
        if i == 2:
            feature_send(mirror, buddy, heads - 3)
        x = xbuf[src]
        g = gain[pl.ds(src * levels + me_l, 1), :]
        acc += lax.dot_general(
            (x * g).astype(jnp.bfloat16), wbuf[src], (((1,), (1 if flipped else 0,)), ((), ())),
            preferred_element_type=jnp.float32)
        squares += jnp.sum(x * x, axis=1, keepdims=True)

    for g in order:
        state_copy(g).start()
    ow_copy.start()

    proj[:, :cols] = acc
    lane = lax.broadcasted_iota(jnp.int32, (seqs, LANES), 1)
    tail0 = 2 * key_dim + 2 * val_dim
    tail = jnp.where(lane < level_total, proj[:, tail0 : tail0 + LANES], 0.0)
    tail = jnp.where(lane == level_total, squares, tail)
    pack = tail[:packed]
    for c in range(1, slots):
        pack += pltpu.roll(tail[c * packed : (c + 1) * packed], slot * c, 1)
    abuf[me_l, :seqs, :] = acc[:, :key_dim]
    abuf[me_l, seqs:, :] = pack
    for o in range(1, levels):
        peer = lax.rem(me_l + o, levels)
        c = send(abuf.at[me_l], abuf.at[me_l], a_send.at[o], a_recv.at[me_l], (me_h, peer))
        c.start()
        pending.append(c)
    for o in range(1, levels):
        peer = lax.rem(me_l + o, levels)
        rows = pl.ds(pl.multiple_of(peer * owned, owned), owned)
        c = send(proj.at[rows, pl.ds(key_dim, tail0 - key_dim)], bbuf.at[me_l],
                 b_send.at[o], b_recv.at[me_l], (me_h, peer))
        c.start()
        pending.append(c)
    mine = pl.ds(pl.multiple_of(me_l * owned, owned), owned)
    bbuf[me_l] = proj[mine, key_dim:tail0]

    biasbuf[:, :level_total] = bias[...]
    row = lax.broadcasted_iota(jnp.int32, (seqs, seqs), 0)
    col = lax.broadcasted_iota(jnp.int32, (seqs, seqs), 1)
    pos_f = jnp.broadcast_to(pos[...], (seqs, seqs)).astype(jnp.float32)
    pos_col = jnp.sum(jnp.where(row == col, pos_f, 0.0), axis=1, keepdims=True).astype(jnp.int32)
    shift = jnp.clip(lane - 1, 0, 31)
    bits = jnp.bitwise_and(jnp.right_shift(jnp.broadcast_to(pos_col, lane.shape), shift), 1)
    occupied = jnp.logical_and(lane < level_total, jnp.logical_or(lane == 0, bits == 1))

    for o in range(1, levels):
        src = lax.rem(me_l + levels - o, levels)
        send(abuf.at[src], abuf.at[src], a_send.at[o], a_recv.at[src], (me_h, src)).wait_recv()
    query = abuf[0, :seqs, :]
    pack = abuf[0, seqs:, :]
    for l in range(1, levels):
        query += abuf[l, :seqs, :]
        pack += abuf[l, seqs:, :]
    parts = [pack] + [pltpu.roll(pack, LANES - slot * c, 1) for c in range(1, slots)]
    tail = jnp.concatenate(parts, axis=0)
    row_scale = lax.rsqrt(tail[:, level_total : level_total + 1] / width + 1e-06)
    query = query * row_scale
    logits = tail * row_scale + biasbuf[...]
    peak = jnp.max(jnp.where(occupied, logits, -1e30), axis=1, keepdims=True)
    weights = jnp.where(occupied, jnp.exp(logits - peak), 0.0)
    weights = weights / jnp.sum(weights, axis=1, keepdims=True)
    qfull[...] = query
    wnorm[:, :LANES] = weights
    wnorm[:, LANES:] = jnp.broadcast_to(row_scale, weights.shape)
    local = pltpu.roll(weights, lax.rem(LANES - me_l * level_here, LANES), 1)
    query_low = query.astype(jnp.bfloat16).astype(jnp.float32)
    for j in range(level_here):
        qw[:, j * key_dim : (j + 1) * key_dim] = (query_low * local[:, j : j + 1]).astype(jnp.bfloat16)

    seq_in = lax.broadcasted_iota(jnp.int32, (GROUP, val_dim), 0)
    def to_levels(rows, index):
        for o in range(1, levels):
            part = mbuf.at[me_l, rows, :]
            c = send(part, part, m_send.at[o, index], m_recv.at[me_l, index],
                     (me_h, lax.rem(me_l + o, levels)))
            c.start()
            pending.append(c)

    for t, g in enumerate(order):
        if t == groups - 1:
            for o in range(1, levels):
                src = lax.rem(me_l + levels - o, levels)
                send(bbuf.at[src], bbuf.at[src], b_send.at[o], b_recv.at[src], (me_h, src)).wait_recv()
            rest = bbuf[0]
            for l in range(1, levels):
                rest += bbuf[l]
            rest = rest * wnorm[mine, LANES : LANES + 1]
            key, value = rest[:, :key_dim], rest[:, key_dim : key_dim + val_dim]
            gate = rest[:, key_dim + val_dim :]
            own = jnp.sum(qfull[mine, :] * key, axis=1, keepdims=True) * key_dim ** (-0.5) * value
            mbuf[me_l, seqs:, :] = gate * jax.nn.sigmoid(gate)
            to_levels(pl.ds(seqs, owned), groups)
            qfull[...] = jnp.zeros(qfull.shape, jnp.float32)
            qfull[mine, :] = wnorm[mine, 0:1] * own
        state_copy(g).wait()
        base = pl.multiple_of(g * GROUP, GROUP)
        rows = pl.ds(base, GROUP)
        left = qw[rows, :]
        mixed = jnp.zeros((GROUP, val_dim), jnp.float32)
        for i in range(GROUP):
            got = jnp.dot(left, sbuf[base + i], preferred_element_type=jnp.float32)
            mixed = jnp.where(seq_in == i, got, mixed)
        if t == groups - 1:
            mixed += qfull[rows, :]
        mbuf[me_l, rows, :] = mixed
        to_levels(rows, g)
    ow_copy.wait()
    for o in range(1, levels):
        src = lax.rem(me_l + levels - o, levels)
        for index in range(groups + 1):
            rows = pl.ds(index * GROUP, GROUP if index < groups else owned)
            part = mbuf.at[src, rows, :]
            send(part, part, m_send.at[o, index], m_recv.at[src, index], (me_h, src)).wait_recv()
    gated = mbuf[0, :seqs, :]
    for l in range(1, levels):
        gated += mbuf[l, :seqs, :]
    gated = gated * jnp.concatenate([mbuf[l, seqs:, :] for l in range(levels)], axis=0)
    total_sq = jnp.sum(gated * gated, axis=1, keepdims=True)
    product = jnp.dot((gated * ogain[...]).astype(jnp.bfloat16), owbuf[...], preferred_element_type=jnp.float32)
    qsum[me_h] = jnp.sum(jnp.where(row == col, jnp.broadcast_to(total_sq, (seqs, seqs)), 0.0), axis=0, keepdims=True)
    for h in range(heads):
        osend[h] = product[h * out_rows : (h + 1) * out_rows]
    for o in range(1, heads):
        peer = lax.rem(me_h + o, heads)
        c = send(osend.at[peer], orecv.at[me_h], o_send.at[o], o_recv.at[me_h], (peer, me_l))
        c.start()
        pending.append(c)
        c = send(qsum.at[me_h], qsum.at[me_h], q_send.at[o], q_recv.at[me_h], (peer, me_l))
        c.start()
        pending.append(c)
    total = osend[me_h]
    for o in range(1, heads):
        src = lax.rem(me_h + heads - o, heads)
        send(osend.at[src], orecv.at[src], o_send.at[o], o_recv.at[src], (src, me_l)).wait_recv()
        send(qsum.at[src], qsum.at[src], q_send.at[o], q_recv.at[src], (src, me_l)).wait_recv()
        total += orecv[src]
    all_sq = qsum[0]
    for h in range(1, heads):
        all_sq += qsum[h]
    here = lax.broadcasted_iota(jnp.int32, (out_rows, seqs), 0) + me_h * out_rows
    pick = lax.broadcasted_iota(jnp.int32, (out_rows, seqs), 1) == here
    mean = jnp.sum(jnp.where(pick, jnp.broadcast_to(all_sq, pick.shape), 0.0), axis=1, keepdims=True) / (heads * val_dim)
    out[...] = total * lax.rsqrt(mean + 1e-05)
    for c in pending:
        c.wait_send()


def body(features, in_gain, in_weight, level_bias, states, positions, out_gain, out_weight):
    heads, levels = lax.axis_size("head"), lax.axis_size("level")
    seqs, fw = features.shape
    cols = in_weight.shape[1]
    _, head_here, level_here, key_dim, val_dim = states.shape
    level_total = level_bias.shape[1]
    assert head_here == 1 and key_dim == LANES and val_dim == LANES
    out_cols = out_weight.shape[1]
    flipped = fw % LANES == 0
    slots = LANES // (1 << level_total.bit_length())
    owned, out_rows = seqs // levels, seqs // heads
    f32, bf16 = jnp.float32, jnp.bfloat16
    vmem, anyspace = pl.BlockSpec(memory_space=pltpu.VMEM), pl.BlockSpec(memory_space=pl.ANY)
    dma = pltpu.SemaphoreType.DMA
    tail0 = 2 * key_dim + 2 * val_dim
    return pl.pallas_call(
        functools.partial(kernel, heads, levels, in_gain.shape[0], (key_dim, val_dim, level_total, level_here)),
        out_shape=pltpu.VMEM((out_rows, out_cols), f32),
        in_specs=[anyspace, vmem, anyspace, vmem, anyspace, vmem, vmem, anyspace],
        out_specs=vmem,
        scratch_shapes=[
            pltpu.VMEM((heads, seqs, fw), f32),
            pltpu.VMEM((heads, cols, fw) if flipped else (heads, fw, cols), bf16),
            pltpu.VMEM((seqs, level_here * key_dim, val_dim), bf16),
            pltpu.VMEM(out_weight.shape, bf16),
            pltpu.VMEM((seqs, tail0 + LANES), f32),
            pltpu.VMEM((levels, seqs + seqs // slots, key_dim), f32),
            pltpu.VMEM((levels, owned, tail0 - key_dim), f32),
            pltpu.VMEM((levels, seqs + owned, val_dim), f32),
            pltpu.VMEM((heads, out_rows, out_cols), f32),
            pltpu.VMEM((heads, out_rows, out_cols), f32),
            pltpu.VMEM((seqs, key_dim), f32),
            pltpu.VMEM((seqs, 2 * LANES), f32),
            pltpu.VMEM((seqs, level_here * key_dim), bf16),
            pltpu.VMEM((1, LANES), f32),
            pltpu.VMEM((heads, 1, seqs), f32),
            dma(()), dma((heads,)), dma((seqs // GROUP,)), dma(()),
            dma((heads,)), dma((heads,)),
            dma((levels,)), dma((levels,)), dma((levels,)), dma((levels,)),
            dma((levels, seqs // GROUP + 1)), dma((levels, seqs // GROUP + 1)),
            dma((heads,)), dma((heads,)), dma((heads,)), dma((heads,)),
        ],
        compiler_params=pltpu.CompilerParams(collective_id=0, has_side_effects=True),
    )(
        features,
        in_gain.reshape(heads * levels, fw),
        in_weight.T if flipped else in_weight,
        level_bias,
        states.reshape(seqs, level_here * key_dim, val_dim),
        positions.reshape(1, seqs),
        out_gain.reshape(1, val_dim),
        out_weight,
    )


def solution(mesh):
    in_specs = (
        P(None, ("head", "level")),
        P(),
        P(None, "head"),
        P("head", None),
        P(None, "head", "level", None, None),
        P(),
        P("head"),
        P("head", "level"),
    )
    out_specs = P("head", "level")
    return jax.shard_map(body, mesh=mesh, in_specs=in_specs, out_specs=out_specs, check_vma=False)
```
